768 devices in a mesh: dp: 48 (over z, y_hi), expert: 16 (over x, y_lo, core).
Axes of the slice: x: 4, y: 8 (y_hi: 4, y_lo: 2; y = y_hi * 2 + y_lo), z: 12, core: 2. Of those that a mesh axis runs over, the one named last changes fastest.
Arguments:
- queries: bfloat16 [24576, 4096], P('dp', 'expert'), may hold values from -6 to 6
- key_states: bfloat16 [24576, 4096], P('dp', 'expert'), may hold values from -6 to 6
- value_states: bfloat16 [24576, 4096], P('dp', 'expert'), may hold values from -6 to 6
- doc_lengths: int32 [48, 8], replicated, may hold values from 0 to 512, as said below
- move_plan: int32 [48, 2], replicated, may hold values from 0 to 47, as said below
- expert_ids: int32 [24576, 8], P('dp'), may hold values from 0 to 15, all different within a row; in each aligned block of 512 rows (0 to 511, 512 to 1023, ...) at most 384 rows name the same one
- gate_weights: float32 [24576, 8], P('dp'), may hold values from 0.05 to 0.5
- expert_weight: bfloat16 [16, 4096, 1024], P('expert'), may hold values from -0.29882812 to 0.29882812
Outputs:
- attended: bfloat16 [24576, 4096], P('dp', 'expert')
- combined: bfloat16 [24576, 1024], P('dp', 'expert')
- row_load: float32 [48], P('dp')
The draws below stay inside these ranges and needn't reach their ends.
Inputs may be any that keep to these rules, and one draw needn't show every extreme that they name: `doc_lengths`: each row's entries are the lengths of its packed documents in order and sum to 512; a zero marks an absent document; some row holds a single document. move_plan[r, 0] is r itself or the row half the dp axis away, (r + 48 / 2) mod 48; a row is handed to its partner only if its pairs in all exceed the partner's, so two partners never both move; move_plan[r, 1] is a block number below 2; at least one row moves a block. `expert_ids`: each token names 8 different experts; among the 512 tokens of one row no expert is named by more than 384 tokens.
All inputs are finite; a program needn't handle non-finite values.
Results may differ from the reference program's by a relative error of at most 0.0095.
Values may be sent and summed in bfloat16 or wider, within the bound.
No kernel may reach another device: no remote copies, remote signals or barrier semaphores. Data moves between devices by JAX's collectives and lax.ppermute only.
A program may use at most 64 MiB of HBM per device.

```python
import math
import jax
import jax.numpy as jnp
import numpy as np
from jax import lax

HEADS = 32
HEAD_DIM = 128
QBLOCK = 128
BLOCKS = 4
MAX_DOCS = 8
EXPERT_FF = 1024
EXPERTS = 16
TOPK = 8
ROW_TOKENS = 512
TOKENS = 24576
D_ATT = 4096
CAP = 384
N_DP = 48


def joint_states(key):
    first = jax.random.normal(jax.random.fold_in(key, 11), (TOKENS, D_ATT), jnp.float32)
    second = jax.random.normal(jax.random.fold_in(key, 12), (TOKENS, D_ATT), jnp.float32)
    first = jnp.clip(first, -6.0, 6.0)
    second = jnp.clip(second, -6.0, 6.0)
    return (first, second)


def draw_queries(key, part):
    return joint_states(key)[0].astype(jnp.bfloat16)


def draw_key_states(key, part):
    return joint_states(key)[1].astype(jnp.bfloat16)


def lengths_table(key):
    row_ids = jnp.arange(N_DP, dtype=jnp.int32)
    counts = jax.random.randint(jax.random.fold_in(key, 21), (N_DP, 1), 1, MAX_DOCS + 1)
    single = jax.random.randint(jax.random.fold_in(key, 22), (), 0, N_DP)
    counts = jnp.where(row_ids[:, None] == single, 1, counts)
    raw_cuts = jax.random.randint(jax.random.fold_in(key, 23), (N_DP, MAX_DOCS - 1), 1, ROW_TOKENS)
    used = jnp.arange(MAX_DOCS - 1, dtype=jnp.int32)[None, :] < counts - 1
    cuts = jnp.sort(jnp.where(used, raw_cuts, ROW_TOKENS), axis=1)
    edges = jnp.concatenate([jnp.zeros((N_DP, 1), jnp.int32), cuts.astype(jnp.int32), jnp.full((N_DP, 1), ROW_TOKENS, jnp.int32)], 1)
    return (edges[:, 1:] - edges[:, :-1]).astype(jnp.int32)


def draw_doc_lengths(key, part):
    return lengths_table(key)


def draw_move_plan(key, part):
    lengths = lengths_table(key)
    bounds = jnp.cumsum(lengths, axis=1).astype(jnp.int32)
    positions = jnp.arange(ROW_TOKENS, dtype=jnp.int32)
    starts = jnp.max(jnp.where(bounds[:, None, :] <= positions[None, :, None], bounds[:, None, :], 0), axis=2)
    pairs = (positions[None, :] - starts + 1).reshape(N_DP, BLOCKS, QBLOCK).sum(axis=2)
    totals = jnp.sum(pairs, axis=1)
    row_ids = jnp.arange(N_DP, dtype=jnp.int32)
    partner = (row_ids + N_DP // 2) % N_DP
    moves = totals > totals[partner]
    heavy = jnp.argmax(totals).astype(jnp.int32)
    moves = jnp.where(jnp.any(moves), moves, row_ids == heavy)
    blocks = jnp.argmax(pairs[:, :BLOCKS // 2], axis=1).astype(jnp.int32)
    runner = jnp.where(moves, partner, row_ids)
    return jnp.stack([runner, blocks], 1).astype(jnp.int32)


def shard_levels(own_key, extent, cuts, smallest, largest):
    gain = 1.0
    for axis_at, parts in cuts:
        steps = jax.random.uniform(jax.random.fold_in(jax.random.fold_in(own_key, 6), axis_at), (parts,), jnp.float32, smallest / len(cuts), largest / len(cuts))
        gain = gain * jnp.repeat(jnp.exp(steps), extent[axis_at] // parts).reshape((-1,) + (1,) * (len(extent) - 1 - axis_at))
    return gain


def routed_block(stream_key, own, number, rows, count, top, reach, slope):
    ranking = jax.random.permutation(stream_key, count)
    crowded, usual = portions_of(count, rows * top, reach, slope, True), portions_of(count, rows * top, reach, slope, False)
    places = jnp.arange(count)

    def named(tallies, offset_by):
        used = int((tallies > 0).sum())
        fixed = max(1, used // 4)
        passed = fixed + (places - fixed + offset_by * (used - fixed)) % max(1, count - fixed)
        return jnp.zeros((count,), jnp.int32).at[ranking[jnp.where(places < fixed, places, passed)]].set(jnp.asarray(tallies, jnp.int32))

    tallies = jnp.where(number % 4 == 0, named(crowded, number // 4), named(usual, number - number // 4 - 1))
    mixed = jax.random.permutation(jax.random.fold_in(own, 3), count)
    source_of, receiver = mixed[0:count // 2 * 2:2], mixed[1:count // 2 * 2:2]
    slack = jnp.minimum(tallies[source_of] - 1, reach - tallies[receiver]) // 2
    slack = jnp.where((source_of == ranking[0]) | (receiver == ranking[0]) | (tallies[receiver] == 0), 0, jnp.maximum(slack, 0))
    passed = jax.random.randint(jax.random.fold_in(own, 4), (count // 2,), 0, 1 << 20) % (slack + 1)
    tallies = tallies.at[source_of].add(-passed).at[receiver].add(passed)
    labels = jnp.searchsorted(jnp.cumsum(tallies), jnp.arange(rows * top), side="right").astype(jnp.int32)
    listing = labels.reshape(top, rows).T
    listing = listing[jax.random.permutation(jax.random.fold_in(own, 1), rows)]
    offset_by = jax.random.randint(jax.random.fold_in(own, 2), (rows, 1), 0, top)
    return jnp.take_along_axis(listing, (jnp.arange(top)[None, :] + offset_by) % top, axis=1)


def portions_of(count, total, most, skew, full):
    weights = [(1 << 20) // math.isqrt(grade ** skew) + 1 for grade in range(1, count + 1)]
    largest = most if full else min(most, max(-(-total // count), total * weights[0] // sum(weights)))
    least = 1 if total - largest >= count - 1 else 0
    given, rest = [largest] + [least] * (count - 1), total - largest - least * (count - 1)
    while rest > 0:
        movable = [i for i in range(1, count) if given[i] < largest] or [i for i in range(1, count) if given[i] < most]
        pool, remaining = sum([weights[i] for i in movable]), rest
        for i in movable:
            more = min(most - given[i], max(1, remaining * weights[i] // pool), rest)
            given[i] = given[i] + more
            rest = rest - more
    return np.array(given)


def scatter_about(stream_key, extent, scale, most, cuts=(), kind=jnp.bfloat16):
    entries = jax.random.normal(stream_key, extent, jnp.float32) * scale
    if len(cuts) > 0:
        entries = shard_levels(stream_key, extent, cuts, -0.22, 0.18) * entries
    return jnp.clip(entries, min=-most, max=most).astype(kind)


def setup_inputs(seed: int = 0) -> dict:
    streams_of = jax.random.split(jax.random.key(seed), 9)
    queries = draw_queries(jax.random.fold_in(streams_of[8], 71), 0)
    key_states = draw_key_states(jax.random.fold_in(streams_of[8], 71), 0)
    value_states = scatter_about(streams_of[2], (TOKENS, D_ATT), 1.0, 6.0, ((0, 48), (1, 16)))
    doc_lengths = draw_doc_lengths(jax.random.fold_in(streams_of[8], 71), 0)
    move_plan = draw_move_plan(jax.random.fold_in(streams_of[8], 71), 0)
    expert_ids_keys = jax.random.split(jax.random.fold_in(streams_of[5], 1), TOKENS // ROW_TOKENS)
    expert_ids_turns = jax.random.permutation(jax.random.fold_in(streams_of[5], 3), TOKENS // ROW_TOKENS)
    expert_ids = jax.vmap(lambda own, number: routed_block(jax.random.fold_in(streams_of[5], 2), own, number, ROW_TOKENS, EXPERTS, TOPK, CAP, 1))(expert_ids_keys, expert_ids_turns).reshape((TOKENS, TOPK))
    gate_weights = jnp.clip(0.05 + 0.45 * jax.random.uniform(streams_of[6], (TOKENS, TOPK), jnp.float32) ** shard_levels(streams_of[6], (TOKENS, TOPK), ((0, 48),), -0.2, 0.2), 0.05, 0.5)
    expert_weight = scatter_about(streams_of[7], (EXPERTS, D_ATT, EXPERT_FF), 0.05, 0.29882812, ((0, 16),))
    return dict(queries=queries, key_states=key_states, value_states=value_states, doc_lengths=doc_lengths, move_plan=move_plan, expert_ids=expert_ids, gate_weights=gate_weights, expert_weight=expert_weight)


def token_starts(row_lengths, row_count):
    bounds = jnp.cumsum(row_lengths).astype(jnp.int32)
    positions = jnp.arange(row_count, dtype=jnp.int32)
    return jnp.max(jnp.where(bounds[None, :] <= positions[:, None], bounds[None, :], 0), axis=1)


def attend_row(inputs):
    query_rows, key_rows, value_rows, row_lengths = inputs
    starts = token_starts(row_lengths, ROW_TOKENS)
    positions = jnp.arange(ROW_TOKENS, dtype=jnp.int32)
    query_heads = query_rows.astype(jnp.float32).reshape(ROW_TOKENS, HEADS, HEAD_DIM)
    key_heads = key_rows.astype(jnp.float32).reshape(ROW_TOKENS, HEADS, HEAD_DIM)
    value_heads = value_rows.astype(jnp.float32).reshape(ROW_TOKENS, HEADS, HEAD_DIM)
    scores = jnp.einsum("qhd,khd->hqk", query_heads, key_heads) * (HEAD_DIM ** -0.5)
    allowed = (positions[None, :] <= positions[:, None]) & (positions[None, :] >= starts[:, None])
    scores = jnp.where(allowed[None], scores, -jnp.inf)
    weights = jax.nn.softmax(scores, axis=-1).astype(jnp.bfloat16)
    output = jnp.einsum("hqk,khd->qhd", weights.astype(jnp.float32), value_heads)
    return output.reshape(ROW_TOKENS, D_ATT).astype(jnp.bfloat16)


def reference(queries, key_states, value_states, doc_lengths, move_plan, expert_ids, gate_weights, expert_weight):
    attended = lax.map(attend_row, (queries.reshape(N_DP, ROW_TOKENS, D_ATT), key_states.reshape(N_DP, ROW_TOKENS, D_ATT), value_states.reshape(N_DP, ROW_TOKENS, D_ATT), doc_lengths))
    attended = attended.reshape(TOKENS, D_ATT)

    starts = jax.vmap(lambda lengths_row: token_starts(lengths_row, ROW_TOKENS))(doc_lengths)
    positions = jnp.arange(ROW_TOKENS, dtype=jnp.int32)
    pairs = (positions[None, :] - starts + 1).reshape(N_DP, BLOCKS, QBLOCK).sum(axis=2)
    row_ids = jnp.arange(N_DP, dtype=jnp.int32)
    runner = jnp.where(jnp.arange(BLOCKS, dtype=jnp.int32)[None, :] == move_plan[:, 1:2], move_plan[:, 0:1], row_ids[:, None])
    work = jax.ops.segment_sum(pairs.reshape(-1), runner.reshape(-1).astype(jnp.int32), N_DP)
    row_load = work.astype(jnp.float32) / (QBLOCK * QBLOCK)

    padded = jnp.concatenate([attended, jnp.zeros((1, D_ATT), jnp.bfloat16)], 0)

    def expert_step(carry, expert):
        chosen = expert_ids == expert
        picked = jnp.nonzero(jnp.any(chosen, axis=1), size=CAP * N_DP, fill_value=TOKENS)[0].astype(jnp.int32)
        weight_rows = jnp.sum(jnp.where(chosen, gate_weights, 0.0), axis=1)
        weight_rows = jnp.concatenate([weight_rows, jnp.zeros((1,), weight_rows.dtype)])
        pre_act = jnp.dot(padded[picked], expert_weight[expert], preferred_element_type=jnp.float32)
        rounded = lax.optimization_barrier(jax.nn.silu(pre_act).astype(jnp.bfloat16))
        activated = rounded.astype(jnp.float32)
        return carry.at[picked].add(weight_rows[picked][:, None] * activated), None

    summed, _ = lax.scan(expert_step, jnp.zeros((TOKENS + 1, EXPERT_FF), jnp.float32), jnp.arange(EXPERTS, dtype=jnp.int32))
    combined = summed[:TOKENS].astype(jnp.bfloat16)
    return (attended, combined, row_load)
```

```python
import jax
import jax.numpy as jnp
from jax import lax
from jax.experimental import pallas as pl
from jax.experimental.pallas import tpu as pltpu
from jax.sharding import Mesh
from jax.sharding import PartitionSpec as P

HEAD_DIM = 128
QBLOCK = 128
BLOCKS = 4
MAX_DOCS = 8
ROWS = 512
WIDTH = 256
FF = 1024
CHIPS = 8
GROUP = ("x", "y", "c")


VMEM = pl.BlockSpec(memory_space=pltpu.VMEM)
SMEM = pl.BlockSpec(memory_space=pltpu.SMEM)


def starts_at(lengths_ref, row, positions):
    start = jnp.zeros_like(positions)
    bound = jnp.int32(0)
    for j in range(MAX_DOCS):
        bound = bound + lengths_ref[j, row]
        start = jnp.where(positions >= bound, bound, start)
    return start


def attention_kernel(dp_size, lengths_ref, plan_ref, q_ref, k_ref, v_ref, out_ref, load_ref):
    row = lax.axis_index("dp")
    scale = HEAD_DIM ** (-0.5)
    for b in range(BLOCKS):
        low, high = b * QBLOCK, (b + 1) * QBLOCK
        positions = low + lax.broadcasted_iota(jnp.int32, (QBLOCK, QBLOCK), 0)
        start = starts_at(lengths_ref, row, positions)
        start = jnp.concatenate([start] * (b + 1), axis=1) if b else start
        query_at = low + lax.broadcasted_iota(jnp.int32, (QBLOCK, high), 0)
        key_at = lax.broadcasted_iota(jnp.int32, (QBLOCK, high), 1)
        allowed = (key_at <= query_at) & (key_at >= start)
        for h in range(WIDTH // HEAD_DIM):
            cols = slice(h * HEAD_DIM, (h + 1) * HEAD_DIM)
            scores = lax.dot_general(
                q_ref[low:high, cols], k_ref[:high, cols], (((1,), (1,)), ((), ())),
                preferred_element_type=jnp.float32,
            ) * scale
            scores = jnp.where(allowed, scores, -jnp.inf)
            top = jnp.max(scores, axis=1, keepdims=True)
            e = jnp.exp(scores - top)
            total = jnp.sum(e, axis=1, keepdims=True)
            probs = (e * (1.0 / total)).astype(jnp.bfloat16)
            out = jnp.dot(probs, v_ref[:high, cols], preferred_element_type=jnp.float32)
            out_ref[low:high, cols] = out.astype(jnp.bfloat16)
    partner = lax.rem(row + dp_size // 2, dp_size)
    block = lax.broadcasted_iota(jnp.int32, (8, QBLOCK), 0)
    at = block * QBLOCK + lax.broadcasted_iota(jnp.int32, (8, QBLOCK), 1)
    own_reach = at - starts_at(lengths_ref, row, at) + 1
    partner_reach = at - starts_at(lengths_ref, partner, at) + 1
    gone = jnp.where(plan_ref[0, row] != row, plan_ref[1, row], -1)
    came = jnp.where(plan_ref[0, partner] != partner, plan_ref[1, partner], -1)
    work = jnp.where((block < BLOCKS) & (block != gone), own_reach, 0)
    work = work + jnp.where(block == came, partner_reach, 0)
    load_ref[0] = jnp.sum(work.astype(jnp.float32)) / (QBLOCK * QBLOCK)


def attention(lengths, plan, q, k, v, dp_size):
    return pl.pallas_call(
        lambda *refs: attention_kernel(dp_size, *refs),
        out_shape=(
            jax.ShapeDtypeStruct((ROWS, WIDTH), jnp.bfloat16),
            jax.ShapeDtypeStruct((1,), jnp.float32),
        ),
        in_specs=[SMEM, SMEM, VMEM, VMEM, VMEM],
        out_specs=(VMEM, SMEM),
        name="attention",
    )(lengths, plan, q, k, v)


def half_sum(x_ref, w_ref, core, cols):
    total = None
    for j in range(CHIPS):
        part = jnp.dot(x_ref[j], w_ref[j, core, :, cols], preferred_element_type=jnp.float32)
        total = part if total is None else total + part
    return total


def own_half_kernel(x_ref, w_ref, chosen_ref, gates_ref, acc_ref, gate_ref):
    core = lax.axis_index("c")
    for n in range(FF // WIDTH):
        cols = slice(n * WIDTH, (n + 1) * WIDTH)
        acc_ref[:, cols] = half_sum(x_ref, w_ref, core, cols)
    own = jnp.where(chosen_ref[...] == lax.axis_index(GROUP), gates_ref[...], 0.0)
    gate = jnp.broadcast_to(jnp.sum(own, axis=0, keepdims=True), (128, ROWS))
    gate_ref[...] = gate.T


def own_half(x, w, chosen, gates):
    return pl.pallas_call(
        own_half_kernel,
        out_shape=(
            jax.ShapeDtypeStruct((ROWS, FF), jnp.float32),
            jax.ShapeDtypeStruct((ROWS, 128), jnp.float32),
        ),
        in_specs=[VMEM] * 4,
        out_specs=(VMEM, VMEM),
        cost_estimate=pl.CostEstimate(
            flops=2 * ROWS * FF * WIDTH * CHIPS, transcendentals=0, bytes_accessed=8 << 20
        ),
        name="own_half",
    )(x, w, chosen, gates)


def other_half_kernel(x_ref, w_ref, own_ref, gate_ref, mine_ref, theirs_ref):
    core = lax.axis_index("c")
    left = lax.broadcasted_iota(jnp.int32, (ROWS // 2, 128), 1) < 64
    gate = gate_ref[...]
    for n in range(FF // WIDTH):
        cols = slice(n * WIDTH, (n + 1) * WIDTH)
        total = own_ref[:, cols] + half_sum(x_ref, w_ref, 1 - core, cols)
        for half in range(WIDTH // 128):
            pre = total[:, half * 128 : (half + 1) * 128]
            act = gate * (pre / (1.0 + jnp.exp(-pre)))
            top, low = act[: ROWS // 2], act[ROWS // 2 :]
            first = jnp.where(left, top, pltpu.roll(low, 64, 1)).astype(jnp.bfloat16)
            second = jnp.where(left, pltpu.roll(top, 64, 1), low).astype(jnp.bfloat16)
            j = n * (WIDTH // 128) + half

            @pl.when(core == 0)
            def _():
                mine_ref[j] = first
                theirs_ref[j] = second

            @pl.when(core != 0)
            def _():
                mine_ref[j] = second
                theirs_ref[j] = first


def other_half(x, w, own, gate):
    return pl.pallas_call(
        other_half_kernel,
        out_shape=(jax.ShapeDtypeStruct((CHIPS, ROWS // 2, 128), jnp.bfloat16),) * 2,
        in_specs=[VMEM] * 4,
        out_specs=(VMEM, VMEM),
        cost_estimate=pl.CostEstimate(
            flops=2 * ROWS * FF * WIDTH * CHIPS, transcendentals=0, bytes_accessed=8 << 20
        ),
        name="other_half",
    )(x, w, own, gate)


def pair_sum_kernel(a_ref, b_ref, out_ref):
    total = a_ref[...].astype(jnp.float32) + b_ref[...].astype(jnp.float32)
    out_ref[...] = total.astype(jnp.bfloat16)


def pair_sum(a, b):
    return pl.pallas_call(
        pair_sum_kernel,
        out_shape=jax.ShapeDtypeStruct(a.shape, jnp.bfloat16),
        in_specs=[VMEM, VMEM],
        out_specs=VMEM,
        name="pair_sum",
    )(a, b)


def gather_sum_kernel(x_ref, out_ref):
    total = x_ref[0].astype(jnp.float32)
    for j in range(1, CHIPS):
        total = total + x_ref[j].astype(jnp.float32)
    turned = total.T.astype(jnp.bfloat16)
    out_ref[:, : ROWS // 2] = turned[:64]
    out_ref[:, ROWS // 2 :] = turned[64:]


def gather_sum(x):
    return pl.pallas_call(
        gather_sum_kernel,
        out_shape=jax.ShapeDtypeStruct((64, ROWS), jnp.bfloat16),
        in_specs=[VMEM],
        out_specs=VMEM,
        name="gather_sum",
    )(x)


def shards(
    queries,
    key_states,
    value_states,
    doc_lengths,
    move_plan,
    expert_ids,
    gate_weights,
    expert_weight,
):
    dp_size = lax.axis_size("dp")
    swap = [(0, 1), (1, 0)]
    attended, row_load = attention(
        doc_lengths.T, move_plan.T, queries, key_states, value_states, dp_size
    )
    weight = expert_weight.reshape(CHIPS, 2, WIDTH, FF)
    own_rows = lax.all_to_all(
        jnp.broadcast_to(attended[None], (CHIPS, ROWS, WIDTH)), ("x", "y"), 0, 0
    )
    other_rows = lax.ppermute(own_rows, "c", swap)
    acc, gate = own_half(own_rows, weight, expert_ids.T, gate_weights.T)
    mine, theirs = other_half(other_rows, weight, acc, gate)
    paired = pair_sum(mine, lax.ppermute(theirs, "c", swap))
    combined = gather_sum(lax.all_to_all(paired, ("x", "y"), 0, 0)).T
    return (attended, combined, row_load)


def solution(mesh):
    split = Mesh(mesh.devices.reshape(mesh.shape["dp"], 4, 2, 2), ("dp",) + GROUP)
    return jax.shard_map(
        shards,
        mesh=split,
        in_specs=(
            P("dp", GROUP),
            P("dp", GROUP),
            P("dp", GROUP),
            P(),
            P(),
            P("dp", None),
            P("dp", None),
            P(GROUP, None, None),
        ),
        out_specs=(P("dp", GROUP), P("dp", GROUP), P("dp")),
        check_vma=False,
    )
```

```python
import jax
import jax.numpy as jnp
from jax import lax
from jax.experimental import pallas as pl
from jax.experimental.pallas import tpu as pltpu
from jax.sharding import Mesh
from jax.sharding import PartitionSpec as P

HEAD_DIM = 128
QBLOCK = 128
BLOCKS = 4
MAX_DOCS = 8
ROWS = 512
WIDTH = 256
FF = 1024
CHIPS = 8
GROUP = ("x", "y", "c")


VMEM = pl.BlockSpec(memory_space=pltpu.VMEM)
SMEM = pl.BlockSpec(memory_space=pltpu.SMEM)
HBM = pl.BlockSpec(memory_space=pltpu.HBM)


def on_chip(*arrays):
    return tuple(pltpu.with_memory_space_constraint(a, pltpu.VMEM) for a in arrays)


def in_hbm(*arrays):
    return tuple(pltpu.with_memory_space_constraint(a, pltpu.HBM) for a in arrays)


def room(mib):
    return pltpu.CompilerParams(vmem_limit_bytes=mib << 20)


def starts_at(lengths_ref, row, positions):
    start = jnp.zeros_like(positions)
    bound = jnp.int32(0)
    for j in range(MAX_DOCS):
        bound = bound + lengths_ref[j, row]
        start = jnp.where(positions >= bound, bound, start)
    return start


def work_tally(dp_size, row, lengths_ref, plan_ref, load_ref):
    partner = lax.rem(row + dp_size // 2, dp_size)
    block = lax.broadcasted_iota(jnp.int32, (8, QBLOCK), 0)
    at = block * QBLOCK + lax.broadcasted_iota(jnp.int32, (8, QBLOCK), 1)
    own_reach = at - starts_at(lengths_ref, row, at) + 1
    partner_reach = at - starts_at(lengths_ref, partner, at) + 1
    gone = jnp.where(plan_ref[0, row] != row, plan_ref[1, row], -1)
    came = jnp.where(plan_ref[0, partner] != partner, plan_ref[1, partner], -1)
    work = jnp.where((block < BLOCKS) & (block != gone), own_reach, 0)
    work = work + jnp.where(block == came, partner_reach, 0)
    load_ref[0] = jnp.sum(work.astype(jnp.float32)) / (QBLOCK * QBLOCK)


def attention_kernel(
    dp_size, lengths_ref, plan_ref, q_hbm, k_hbm, v_hbm, w_hbm, out_ref, load_ref, w_ref,
    q_ref, k_ref, v_ref, sems,
):
    copies = [
        pltpu.make_async_copy(src, dst, sems.at[i])
        for i, (src, dst) in enumerate(
            ((q_hbm, q_ref), (k_hbm, k_ref), (v_hbm, v_ref), (w_hbm, w_ref))
        )
    ]
    for copy in copies:
        copy.start()
    row = lax.axis_index("dp")
    work_tally(dp_size, row, lengths_ref, plan_ref, load_ref)
    for copy in copies[:3]:
        copy.wait()
    scale = HEAD_DIM ** (-0.5)
    for b in range(BLOCKS):
        low, high = b * QBLOCK, (b + 1) * QBLOCK
        positions = low + lax.broadcasted_iota(jnp.int32, (QBLOCK, QBLOCK), 0)
        start = starts_at(lengths_ref, row, positions)
        start = jnp.concatenate([start] * (b + 1), axis=1) if b else start
        query_at = low + lax.broadcasted_iota(jnp.int32, (QBLOCK, high), 0)
        key_at = lax.broadcasted_iota(jnp.int32, (QBLOCK, high), 1)
        allowed = (key_at <= query_at) & (key_at >= start)
        for h in range(WIDTH // HEAD_DIM):
            cols = slice(h * HEAD_DIM, (h + 1) * HEAD_DIM)
            scores = lax.dot_general(
                q_ref[low:high, cols], k_ref[:high, cols], (((1,), (1,)), ((), ())),
                preferred_element_type=jnp.float32,
            ) * scale
            scores = jnp.where(allowed, scores, -jnp.inf)
            top = jnp.max(scores, axis=1, keepdims=True)
            e = jnp.exp(scores - top)
            total = jnp.sum(e, axis=1, keepdims=True)
            probs = (e * (1.0 / total)).astype(jnp.bfloat16)
            out = jnp.dot(probs, v_ref[:high, cols], preferred_element_type=jnp.float32)
            out_ref[low:high, cols] = out.astype(jnp.bfloat16)
    copies[3].wait()


def attention(lengths, plan, q, k, v, w, dp_size):
    return pl.pallas_call(
        lambda *refs: attention_kernel(dp_size, *refs),
        out_shape=(
            pltpu.VMEM((ROWS, WIDTH), jnp.bfloat16),
            jax.ShapeDtypeStruct((1,), jnp.float32),
            pltpu.VMEM(w.shape, jnp.bfloat16),
        ),
        in_specs=[SMEM, SMEM, HBM, HBM, HBM, HBM],
        out_specs=(VMEM, SMEM, VMEM),
        scratch_shapes=[pltpu.VMEM((ROWS, WIDTH), jnp.bfloat16)] * 3
        + [pltpu.SemaphoreType.DMA((4,))],
        compiler_params=room(16),
        name="attention",
    )(*in_hbm(lengths, plan, q, k, v, w))


def half_sum(x_ref, w_ref, core, cols):
    rows = jnp.concatenate([x_ref[j] for j in range(CHIPS)], axis=1)
    columns = w_ref[:, core, :, cols].reshape(CHIPS * WIDTH, WIDTH)
    return jnp.dot(rows, columns, preferred_element_type=jnp.float32)


def own_half_kernel(x_ref, w_ref, chosen_ref, gates_ref, acc_ref, gate_ref):
    core = lax.axis_index("c")
    for n in range(FF // WIDTH):
        cols = slice(n * WIDTH, (n + 1) * WIDTH)
        acc_ref[:, cols] = half_sum(x_ref, w_ref, core, cols)
    own = jnp.where(chosen_ref[...] == lax.axis_index(GROUP), gates_ref[...], 0.0)
    gate = jnp.broadcast_to(jnp.sum(own, axis=0, keepdims=True), (128, ROWS))
    gate_ref[...] = gate.T


def own_half(x, w, chosen, gates):
    return pl.pallas_call(
        own_half_kernel,
        out_shape=(
            pltpu.VMEM((ROWS, FF), jnp.float32),
            pltpu.VMEM((ROWS, 128), jnp.float32),
        ),
        compiler_params=room(20),
        in_specs=[VMEM] * 4,
        out_specs=(VMEM, VMEM),
        cost_estimate=pl.CostEstimate(
            flops=2 * ROWS * FF * WIDTH * CHIPS, transcendentals=0, bytes_accessed=8 << 20
        ),
        name="own_half",
    )(*on_chip(x, w), chosen, gates)


def other_half_kernel(x_ref, w_ref, own_ref, gate_ref, mine_ref, theirs_ref):
    core = lax.axis_index("c")
    left = lax.broadcasted_iota(jnp.int32, (ROWS // 2, 128), 1) < 64
    half_gate = 0.5 * gate_ref[...]
    for n in range(FF // WIDTH):
        cols = slice(n * WIDTH, (n + 1) * WIDTH)
        total = own_ref[:, cols] + half_sum(x_ref, w_ref, 1 - core, cols)
        for half in range(WIDTH // 128):
            pre = total[:, half * 128 : (half + 1) * 128]
            act = half_gate * (pre + pre * jnp.tanh(0.5 * pre))
            top, low = act[: ROWS // 2], act[ROWS // 2 :]
            first = jnp.where(left, top, pltpu.roll(low, 64, 1)).astype(jnp.bfloat16)
            second = jnp.where(left, pltpu.roll(top, 64, 1), low).astype(jnp.bfloat16)
            j = n * (WIDTH // 128) + half

            mine_ref[j] = jnp.where(core == 0, first, second)
            theirs_ref[j] = jnp.where(core == 0, second, first)


def other_half(x, w, own, gate):
    return pl.pallas_call(
        other_half_kernel,
        out_shape=(pltpu.VMEM((CHIPS, ROWS // 2, 128), jnp.bfloat16),) * 2,
        compiler_params=room(20),
        in_specs=[VMEM] * 4,
        out_specs=(VMEM, VMEM),
        cost_estimate=pl.CostEstimate(
            flops=2 * ROWS * FF * WIDTH * CHIPS, transcendentals=0, bytes_accessed=8 << 20
        ),
        name="other_half",
    )(*on_chip(x, w, own, gate))


def pair_sum_kernel(a_ref, b_ref, out_ref):
    total = a_ref[...].astype(jnp.float32) + b_ref[...].astype(jnp.float32)
    out_ref[...] = total.astype(jnp.bfloat16)


def pair_sum(a, b):
    return pl.pallas_call(
        pair_sum_kernel,
        out_shape=pltpu.VMEM(a.shape, jnp.bfloat16),
        compiler_params=room(12),
        in_specs=[VMEM, VMEM],
        out_specs=VMEM,
        name="pair_sum",
    )(*on_chip(a, b))


def gather_sum_kernel(x_ref, out_ref):
    total = x_ref[0].astype(jnp.float32)
    for j in range(1, CHIPS):
        total = total + x_ref[j].astype(jnp.float32)
    turned = total.T.astype(jnp.bfloat16)
    out_ref[:, : ROWS // 2] = turned[:64]
    out_ref[:, ROWS // 2 :] = turned[64:]


def gather_sum(x):
    return pl.pallas_call(
        gather_sum_kernel,
        out_shape=jax.ShapeDtypeStruct((64, ROWS), jnp.bfloat16),
        compiler_params=room(12),
        in_specs=[VMEM],
        out_specs=VMEM,
        name="gather_sum",
    )(*on_chip(x))


def shards(
    queries,
    key_states,
    value_states,
    doc_lengths,
    move_plan,
    expert_ids,
    gate_weights,
    expert_weight,
):
    dp_size = lax.axis_size("dp")
    swap = [(0, 1), (1, 0)]
    weight = expert_weight.reshape(CHIPS, 2, WIDTH, FF)
    attended, row_load, weight = attention(
        doc_lengths.T, move_plan.T, queries, key_states, value_states, weight, dp_size
    )
    own_rows = lax.all_to_all(
        jnp.broadcast_to(attended[None], (CHIPS, ROWS, WIDTH)), ("x", "y"), 0, 0
    )
    other_rows = lax.ppermute(own_rows, "c", swap)
    acc, gate = own_half(own_rows, weight, expert_ids.T, gate_weights.T)
    mine, theirs = other_half(other_rows, weight, acc, gate)
    paired = pair_sum(mine, lax.ppermute(theirs, "c", swap))
    combined = gather_sum(lax.all_to_all(paired, ("x", "y"), 0, 0)).T
    return (attended, combined, row_load)


def solution(mesh):
    split = Mesh(mesh.devices.reshape(mesh.shape["dp"], 4, 2, 2), ("dp",) + GROUP)
    return jax.shard_map(
        shards,
        mesh=split,
        in_specs=(
            P("dp", GROUP),
            P("dp", GROUP),
            P("dp", GROUP),
            P(),
            P(),
            P("dp", None),
            P("dp", None),
            P(GROUP, None, None),
        ),
        out_specs=(P("dp", GROUP), P("dp", GROUP), P("dp")),
        check_vma=False,
    )
```

```python
import math

import jax
import jax.numpy as jnp
from jax import lax
from jax.experimental import pallas as pl
from jax.experimental.pallas import tpu as pltpu
from jax.sharding import Mesh
from jax.sharding import PartitionSpec as P

HEAD_DIM = 128
QBLOCK = 128
BLOCKS = 4
MAX_DOCS = 8
ROWS = 512
WIDTH = 256
FF = 1024
CHIPS = 8
GROUP = ("x", "y", "c")


VMEM = pl.BlockSpec(memory_space=pltpu.VMEM)
SMEM = pl.BlockSpec(memory_space=pltpu.SMEM)
HBM = pl.BlockSpec(memory_space=pltpu.HBM)


def on_chip(*arrays):
    return tuple(pltpu.with_memory_space_constraint(a, pltpu.VMEM) for a in arrays)


def in_hbm(*arrays):
    return tuple(pltpu.with_memory_space_constraint(a, pltpu.HBM) for a in arrays)


def room(mib):
    return pltpu.CompilerParams(vmem_limit_bytes=mib << 20)


def starts_at(lengths_ref, row, positions):
    start = jnp.zeros_like(positions)
    bound = jnp.int32(0)
    for j in range(MAX_DOCS):
        bound = bound + lengths_ref[j, row]
        start = jnp.where(positions >= bound, bound, start)
    return start


def ends_at(lengths_ref, row, count):
    positions = lax.broadcasted_iota(jnp.int32, (1, count), 1)
    bounds = []
    bound = jnp.int32(0)
    for j in range(MAX_DOCS):
        bound = bound + lengths_ref[j, row]
        bounds.append(bound)
    end = jnp.full((1, count), ROWS, jnp.int32)
    for bound in reversed(bounds):
        end = jnp.where(positions < bound, bound, end)
    return end


def work_tally(row, partner, lengths_ref, plan_ref):
    block = lax.broadcasted_iota(jnp.int32, (8, QBLOCK), 0)
    at = block * QBLOCK + lax.broadcasted_iota(jnp.int32, (8, QBLOCK), 1)
    own_reach = at - starts_at(lengths_ref, row, at) + 1
    partner_reach = at - starts_at(lengths_ref, partner, at) + 1
    gone = jnp.where(plan_ref[0, row] != row, plan_ref[1, row], -1)
    came = jnp.where(plan_ref[0, partner] != partner, plan_ref[1, partner], -1)
    work = jnp.where((block < BLOCKS) & (block != gone), own_reach, 0)
    work = work + jnp.where(block == came, partner_reach, 0)
    return jnp.sum(work.astype(jnp.float32)) / (QBLOCK * QBLOCK)


def attention_kernel(
    dp_size, lengths_hbm, plan_hbm, q_hbm, k_hbm, v_hbm, w_hbm,
    out_ref, all_hbm, load_hbm, w_ref,
    q_ref, k_ref, v_ref, lengths_ref, plan_ref, load_ref, sems, out_sems,
):
    copies = [
        pltpu.make_async_copy(src, dst, sems.at[i])
        for i, (src, dst) in enumerate(
            (
                (lengths_hbm, lengths_ref), (plan_hbm, plan_ref),
                (q_hbm, q_ref), (k_hbm, k_ref), (v_hbm, v_ref), (w_hbm, w_ref),
            )
        )
    ]
    for copy in copies:
        copy.start()
    row = lax.axis_index("dp")
    half = dp_size // 2
    partner = jnp.where(row < half, row + half, row - half)
    for copy in copies[:2]:
        copy.wait()
    load_ref[0] = work_tally(row, partner, lengths_ref, plan_ref)
    load_copy = pltpu.make_async_copy(load_ref, load_hbm, out_sems.at[BLOCKS])
    load_copy.start()
    end = ends_at(lengths_ref, row, ROWS)
    query_at = lax.broadcasted_iota(jnp.int32, (QBLOCK, QBLOCK), 0)
    causal = query_at >= lax.broadcasted_iota(jnp.int32, (QBLOCK, QBLOCK), 1)
    factor = HEAD_DIM ** (-0.5) * math.log2(math.e)
    for copy in copies[2:5]:
        copy.wait()
    writes = []
    for b in range(BLOCKS):
        low, high = b * QBLOCK, (b + 1) * QBLOCK
        masks = [
            query_at < end[:, i * QBLOCK : (i + 1) * QBLOCK] - low for i in range(b + 1)
        ]
        masks[b] = masks[b] & causal
        for h in range(WIDTH // HEAD_DIM):
            cols = slice(h * HEAD_DIM, (h + 1) * HEAD_DIM)
            scores = lax.dot_general(
                q_ref[low:high, cols], k_ref[:high, cols], (((1,), (1,)), ((), ())),
                preferred_element_type=jnp.float32,
            )
            scores = jnp.concatenate(
                [
                    jnp.where(mask, scores[:, i * QBLOCK : (i + 1) * QBLOCK], -jnp.inf)
                    for i, mask in enumerate(masks)
                ],
                axis=1,
            )
            top = jnp.max(scores, axis=1, keepdims=True)
            e = jnp.exp2((scores - top) * factor)
            total = jnp.sum(e, axis=1, keepdims=True)
            probs = (e * (1.0 / total)).astype(jnp.bfloat16)
            out = jnp.dot(probs, v_ref[:high, cols], preferred_element_type=jnp.float32)
            out_ref[low:high, cols] = out.astype(jnp.bfloat16)
        rows = pl.ds(low, QBLOCK)
        writes.append(pltpu.make_async_copy(out_ref.at[rows], all_hbm.at[rows], out_sems.at[b]))
        writes[-1].start()
    for copy in (load_copy, *writes, copies[5]):
        copy.wait()


def attention(lengths, plan, q, k, v, w, dp_size):
    return pl.pallas_call(
        lambda *refs: attention_kernel(dp_size, *refs),
        out_shape=(
            pltpu.VMEM((ROWS, WIDTH), jnp.bfloat16),
            pltpu.HBM((ROWS, WIDTH), jnp.bfloat16),
            pltpu.HBM((1,), jnp.float32),
            pltpu.VMEM(w.shape, jnp.bfloat16),
        ),
        in_specs=[HBM] * 6,
        out_specs=(VMEM, HBM, HBM, VMEM),
        scratch_shapes=[pltpu.VMEM((ROWS, WIDTH), jnp.bfloat16)] * 3
        + [
            pltpu.SMEM(lengths.shape, jnp.int32),
            pltpu.SMEM(plan.shape, jnp.int32),
            pltpu.SMEM((1,), jnp.float32),
            pltpu.SemaphoreType.DMA((6,)),
            pltpu.SemaphoreType.DMA((BLOCKS + 1,)),
        ],
        compiler_params=room(16),
        name="attention",
    )(*in_hbm(lengths, plan, q, k, v, w))


def half_sum(x_ref, w_ref, core, cols):
    rows = jnp.concatenate([x_ref[j] for j in range(CHIPS)], axis=1)
    columns = w_ref[:, core, :, cols].reshape(CHIPS * WIDTH, WIDTH)
    return jnp.dot(rows, columns, preferred_element_type=jnp.float32)


def own_half_kernel(x_ref, w_ref, chosen_ref, gates_ref, acc_ref, gate_ref):
    core = lax.axis_index("c")
    for n in range(FF // WIDTH):
        cols = slice(n * WIDTH, (n + 1) * WIDTH)
        acc_ref[:, cols] = half_sum(x_ref, w_ref, core, cols)
    own = jnp.where(chosen_ref[...] == lax.axis_index(GROUP), gates_ref[...], 0.0)
    gate = jnp.broadcast_to(jnp.sum(own, axis=0, keepdims=True), (128, ROWS))
    gate_ref[...] = gate.T


def own_half(x, w, chosen, gates):
    return pl.pallas_call(
        own_half_kernel,
        out_shape=(
            pltpu.VMEM((ROWS, FF), jnp.float32),
            pltpu.VMEM((ROWS, 128), jnp.float32),
        ),
        compiler_params=room(20),
        in_specs=[VMEM] * 4,
        out_specs=(VMEM, VMEM),
        cost_estimate=pl.CostEstimate(
            flops=2 * ROWS * FF * WIDTH * CHIPS, transcendentals=0, bytes_accessed=8 << 20
        ),
        name="own_half",
    )(*on_chip(x, w), chosen, gates)


def other_half_kernel(x_ref, w_ref, own_ref, gate_ref, mine_ref, theirs_ref):
    core = lax.axis_index("c")
    left = lax.broadcasted_iota(jnp.int32, (ROWS // 2, 128), 1) < 64
    half_gate = 0.5 * gate_ref[...]

    def columns(n):
        cols = slice(n * WIDTH, (n + 1) * WIDTH)
        return own_ref[:, cols] + half_sum(x_ref, w_ref, 1 - core, cols)

    following = columns(0)
    for n in range(FF // WIDTH):
        total = following
        if n + 1 < FF // WIDTH:
            following = columns(n + 1)
        for half in range(WIDTH // 128):
            pre = total[:, half * 128 : (half + 1) * 128]
            act = half_gate * (pre + pre * jnp.tanh(0.5 * pre))
            top, low = act[: ROWS // 2], act[ROWS // 2 :]
            first = jnp.where(left, top, pltpu.roll(low, 64, 1)).astype(jnp.bfloat16)
            second = jnp.where(left, pltpu.roll(top, 64, 1), low).astype(jnp.bfloat16)
            j = n * (WIDTH // 128) + half

            mine_ref[j] = jnp.where(core == 0, first, second)
            theirs_ref[j] = jnp.where(core == 0, second, first)


def other_half(x, w, own, gate):
    return pl.pallas_call(
        other_half_kernel,
        out_shape=(pltpu.VMEM((CHIPS, ROWS // 2, 128), jnp.bfloat16),) * 2,
        compiler_params=room(20),
        in_specs=[VMEM] * 4,
        out_specs=(VMEM, VMEM),
        cost_estimate=pl.CostEstimate(
            flops=2 * ROWS * FF * WIDTH * CHIPS, transcendentals=0, bytes_accessed=8 << 20
        ),
        name="other_half",
    )(*on_chip(x, w, own, gate))


def pair_sum_kernel(a_ref, b_ref, out_ref):
    total = a_ref[...].astype(jnp.float32) + b_ref[...].astype(jnp.float32)
    out_ref[...] = total.astype(jnp.bfloat16)


def pair_sum(a, b):
    return pl.pallas_call(
        pair_sum_kernel,
        out_shape=pltpu.VMEM(a.shape, jnp.bfloat16),
        compiler_params=room(12),
        in_specs=[VMEM, VMEM],
        out_specs=VMEM,
        name="pair_sum",
    )(*on_chip(a, b))


def gather_sum_kernel(x_ref, out_ref):
    total = x_ref[0].astype(jnp.float32)
    for j in range(1, CHIPS):
        total = total + x_ref[j].astype(jnp.float32)
    turned = total.T.astype(jnp.bfloat16)
    out_ref[:, : ROWS // 2] = turned[:64]
    out_ref[:, ROWS // 2 :] = turned[64:]


def gather_sum(x):
    return pl.pallas_call(
        gather_sum_kernel,
        out_shape=jax.ShapeDtypeStruct((64, ROWS), jnp.bfloat16),
        compiler_params=room(12),
        in_specs=[VMEM],
        out_specs=VMEM,
        name="gather_sum",
    )(*on_chip(x))


def shards(
    queries,
    key_states,
    value_states,
    doc_lengths,
    move_plan,
    expert_ids,
    gate_weights,
    expert_weight,
):
    dp_size = lax.axis_size("dp")
    swap = [(0, 1), (1, 0)]
    weight = expert_weight.reshape(CHIPS, 2, WIDTH, FF)
    rows, attended, row_load, weight = attention(
        doc_lengths.T, move_plan.T, queries, key_states, value_states, weight, dp_size
    )
    own_rows = lax.all_to_all(
        jnp.broadcast_to(rows[None], (CHIPS, ROWS, WIDTH)), ("x", "y"), 0, 0
    )
    other_rows = lax.ppermute(own_rows, "c", swap)
    acc, gate = own_half(own_rows, weight, expert_ids.T, gate_weights.T)
    mine, theirs = other_half(other_rows, weight, acc, gate)
    paired = pair_sum(mine, lax.ppermute(theirs, "c", swap))
    combined = gather_sum(lax.all_to_all(paired, ("x", "y"), 0, 0)).T
    return (attended, combined, row_load)


def solution(mesh):
    split = Mesh(mesh.devices.reshape(mesh.shape["dp"], 4, 2, 2), ("dp",) + GROUP)
    return jax.shard_map(
        shards,
        mesh=split,
        in_specs=(
            P("dp", GROUP),
            P("dp", GROUP),
            P("dp", GROUP),
            P(),
            P(),
            P("dp", None),
            P("dp", None),
            P(GROUP, None, None),
        ),
        out_specs=(P("dp", GROUP), P("dp", GROUP), P("dp")),
        check_vma=False,
    )
```

```python
import math

import jax
import jax.numpy as jnp
from jax import lax
from jax.experimental import pallas as pl
from jax.experimental.pallas import tpu as pltpu
from jax.sharding import Mesh
from jax.sharding import PartitionSpec as P

HEAD_DIM = 128
QBLOCK = 128
QTILE = 128
BLOCKS = 4
MAX_DOCS = 8
ROWS = 512
WIDTH = 256
FF = 1024
CHIPS = 8
GROUP = ("x", "y", "c")


VMEM = pl.BlockSpec(memory_space=pltpu.VMEM)
SMEM = pl.BlockSpec(memory_space=pltpu.SMEM)
HBM = pl.BlockSpec(memory_space=pltpu.HBM)


def on_chip(*arrays):
    return tuple(pltpu.with_memory_space_constraint(a, pltpu.VMEM) for a in arrays)


def in_hbm(*arrays):
    return tuple(pltpu.with_memory_space_constraint(a, pltpu.HBM) for a in arrays)


def room(mib):
    return pltpu.CompilerParams(vmem_limit_bytes=mib << 20)


def starts_at(lengths_ref, row, positions):
    start = jnp.zeros_like(positions)
    bound = jnp.int32(0)
    for j in range(MAX_DOCS):
        bound = bound + lengths_ref[j, row]
        start = jnp.where(positions >= bound, bound, start)
    return start


def ends_at(lengths_ref, row, count):
    positions = lax.broadcasted_iota(jnp.int32, (1, count), 1)
    bounds = []
    bound = jnp.int32(0)
    for j in range(MAX_DOCS):
        bound = bound + lengths_ref[j, row]
        bounds.append(bound)
    end = jnp.full((1, count), ROWS, jnp.int32)
    for bound in reversed(bounds):
        end = jnp.where(positions < bound, bound, end)
    return end


def work_tally(row, partner, lengths_ref, plan_ref):
    block = lax.broadcasted_iota(jnp.int32, (8, QBLOCK), 0)
    at = block * QBLOCK + lax.broadcasted_iota(jnp.int32, (8, QBLOCK), 1)
    own_reach = at - starts_at(lengths_ref, row, at) + 1
    partner_reach = at - starts_at(lengths_ref, partner, at) + 1
    gone = jnp.where(plan_ref[0, row] != row, plan_ref[1, row], -1)
    came = jnp.where(plan_ref[0, partner] != partner, plan_ref[1, partner], -1)
    work = jnp.where((block < BLOCKS) & (block != gone), own_reach, 0)
    work = work + jnp.where(block == came, partner_reach, 0)
    return jnp.sum(work.astype(jnp.float32)) / (QBLOCK * QBLOCK)


def attention_kernel(
    dp_size, lengths_hbm, plan_hbm, q_hbm, k_hbm, v_hbm, w_hbm,
    out_ref, load_hbm, w_ref,
    q_ref, k_ref, v_ref, lengths_ref, plan_ref, load_ref, sems, out_sem,
):
    copies = [
        pltpu.make_async_copy(src, dst, sems.at[i])
        for i, (src, dst) in enumerate(
            (
                (lengths_hbm, lengths_ref), (plan_hbm, plan_ref),
                (q_hbm, q_ref), (k_hbm, k_ref), (v_hbm, v_ref),
                *((w_hbm.at[j, lax.axis_index("c")], w_ref.at[j]) for j in range(CHIPS)),
            )
        )
    ]
    for copy in copies:
        copy.start()
    row = lax.axis_index("dp")
    half = dp_size // 2
    partner = jnp.where(row < half, row + half, row - half)
    for copy in copies[:2]:
        copy.wait()
    load_ref[0] = work_tally(row, partner, lengths_ref, plan_ref)
    load_copy = pltpu.make_async_copy(load_ref, load_hbm, out_sem)
    load_copy.start()
    end = ends_at(lengths_ref, row, ROWS)
    query_at = lax.broadcasted_iota(jnp.int32, (QTILE, QBLOCK), 0)
    key_at = lax.broadcasted_iota(jnp.int32, (QTILE, QBLOCK), 1)
    factor = HEAD_DIM ** (-0.5) * math.log2(math.e)
    for copy in copies[2:5]:
        copy.wait()
    for t in range(ROWS // QTILE):
        low, b = t * QTILE, t * QTILE // QBLOCK
        high = (b + 1) * QBLOCK
        masks = [
            query_at < end[:, i * QBLOCK : (i + 1) * QBLOCK] - low for i in range(b + 1)
        ]
        masks[b] = masks[b] & (query_at >= key_at + (b * QBLOCK - low))
        for h in range(WIDTH // HEAD_DIM):
            cols = slice(h * HEAD_DIM, (h + 1) * HEAD_DIM)
            scores = lax.dot_general(
                q_ref[low : low + QTILE, cols], k_ref[:high, cols], (((1,), (1,)), ((), ())),
                preferred_element_type=jnp.float32,
            )
            scores = jnp.concatenate(
                [
                    jnp.where(mask, scores[:, i * QBLOCK : (i + 1) * QBLOCK], -jnp.inf)
                    for i, mask in enumerate(masks)
                ],
                axis=1,
            )
            top = jnp.max(scores, axis=1, keepdims=True)
            e = jnp.exp2((scores - top) * factor)
            total = jnp.sum(e, axis=1, keepdims=True)
            probs = (e * (1.0 / total)).astype(jnp.bfloat16)
            out = jnp.dot(probs, v_ref[:high, cols], preferred_element_type=jnp.float32)
            out_ref[low : low + QTILE, cols] = out.astype(jnp.bfloat16)
    for copy in (load_copy, *copies[5:]):
        copy.wait()


def attention(lengths, plan, q, k, v, w, dp_size):
    return pl.pallas_call(
        lambda *refs: attention_kernel(dp_size, *refs),
        out_shape=(
            pltpu.VMEM((ROWS, WIDTH), jnp.bfloat16),
            pltpu.HBM((1,), jnp.float32),
            pltpu.VMEM((CHIPS, WIDTH, FF), jnp.bfloat16),
        ),
        in_specs=[HBM] * 6,
        out_specs=(VMEM, HBM, VMEM),
        scratch_shapes=[pltpu.VMEM((ROWS, WIDTH), jnp.bfloat16)] * 3
        + [
            pltpu.SMEM(lengths.shape, jnp.int32),
            pltpu.SMEM(plan.shape, jnp.int32),
            pltpu.SMEM((1,), jnp.float32),
            pltpu.SemaphoreType.DMA((5 + CHIPS,)),
            pltpu.SemaphoreType.DMA(()),
        ],
        compiler_params=room(16),
        name="attention",
    )(*in_hbm(lengths, plan, q, k, v, w))


def half_sum(x_ref, w_ref, cols):
    rows = jnp.concatenate([x_ref[j] for j in range(CHIPS)], axis=1)
    columns = w_ref[:, :, cols].reshape(CHIPS * WIDTH, WIDTH)
    return jnp.dot(rows, columns, preferred_element_type=jnp.float32)


def own_half_kernel(
    x_ref, w_ref, rows_ref, w_hbm, chosen_ref, gates_ref,
    acc_ref, gate_ref, rest_ref, all_hbm, sems,
):
    other = 1 - lax.axis_index("c")
    copies = [
        pltpu.make_async_copy(w_hbm.at[j, other], rest_ref.at[j], sems.at[j]) for j in range(CHIPS)
    ]
    copies.append(pltpu.make_async_copy(rows_ref, all_hbm, sems.at[CHIPS]))
    for copy in copies:
        copy.start()
    own = jnp.where(chosen_ref[...] == lax.axis_index(GROUP), gates_ref[...], 0.0)
    gate = jnp.broadcast_to(jnp.sum(own, axis=0, keepdims=True), (128, ROWS))
    gate_ref[...] = gate.T
    for n in range(FF // WIDTH):
        cols = slice(n * WIDTH, (n + 1) * WIDTH)
        acc_ref[:, cols] = half_sum(x_ref, w_ref, cols)
    for copy in copies:
        copy.wait()


def own_half(x, w_own, rows, w, chosen, gates):
    return pl.pallas_call(
        own_half_kernel,
        out_shape=(
            pltpu.VMEM((ROWS, FF), jnp.float32),
            pltpu.VMEM((ROWS, 128), jnp.float32),
            pltpu.VMEM((CHIPS, WIDTH, FF), jnp.bfloat16),
            pltpu.HBM((ROWS, WIDTH), jnp.bfloat16),
        ),
        compiler_params=room(20),
        in_specs=[VMEM, VMEM, VMEM, HBM, VMEM, VMEM],
        out_specs=(VMEM, VMEM, VMEM, HBM),
        scratch_shapes=[pltpu.SemaphoreType.DMA((CHIPS + 1,))],
        cost_estimate=pl.CostEstimate(
            flops=2 * ROWS * FF * WIDTH * CHIPS, transcendentals=0, bytes_accessed=8 << 20
        ),
        name="own_half",
    )(*on_chip(x, w_own, rows), *in_hbm(w), chosen, gates)


def other_half_kernel(x_ref, w_ref, own_ref, gate_ref, mine_ref, theirs_ref):
    core = lax.axis_index("c")
    left = lax.broadcasted_iota(jnp.int32, (ROWS // 2, 128), 1) < 64
    half_gate = 0.5 * gate_ref[...]

    def columns(n):
        cols = slice(n * WIDTH, (n + 1) * WIDTH)
        return own_ref[:, cols] + half_sum(x_ref, w_ref, cols)

    following = columns(0)
    for n in range(FF // WIDTH):
        total = following
        if n + 1 < FF // WIDTH:
            following = columns(n + 1)
        for half in range(WIDTH // 128):
            pre = total[:, half * 128 : (half + 1) * 128]
            act = half_gate * (pre + pre * jnp.tanh(0.5 * pre))
            top, low = act[: ROWS // 2], act[ROWS // 2 :]
            first = jnp.where(left, top, pltpu.roll(low, 64, 1)).astype(jnp.bfloat16)
            second = jnp.where(left, pltpu.roll(top, 64, 1), low).astype(jnp.bfloat16)
            j = n * (WIDTH // 128) + half

            mine_ref[j] = jnp.where(core == 0, first, second)
            theirs_ref[j] = jnp.where(core == 0, second, first)


def other_half(x, w, own, gate):
    return pl.pallas_call(
        other_half_kernel,
        out_shape=(pltpu.VMEM((CHIPS, ROWS // 2, 128), jnp.bfloat16),) * 2,
        compiler_params=room(20),
        in_specs=[VMEM] * 4,
        out_specs=(VMEM, VMEM),
        cost_estimate=pl.CostEstimate(
            flops=2 * ROWS * FF * WIDTH * CHIPS, transcendentals=0, bytes_accessed=8 << 20
        ),
        name="other_half",
    )(*on_chip(x, w, own, gate))


def pair_sum_kernel(a_ref, b_ref, out_ref):
    total = a_ref[...].astype(jnp.float32) + b_ref[...].astype(jnp.float32)
    out_ref[...] = total.astype(jnp.bfloat16)


def pair_sum(a, b):
    return pl.pallas_call(
        pair_sum_kernel,
        out_shape=pltpu.VMEM(a.shape, jnp.bfloat16),
        compiler_params=room(12),
        in_specs=[VMEM, VMEM],
        out_specs=VMEM,
        name="pair_sum",
    )(*on_chip(a, b))


def gather_sum_kernel(x_ref, out_ref):
    total = x_ref[0].astype(jnp.float32)
    for j in range(1, CHIPS):
        total = total + x_ref[j].astype(jnp.float32)
    turned = total.T.astype(jnp.bfloat16)
    out_ref[:, : ROWS // 2] = turned[:64]
    out_ref[:, ROWS // 2 :] = turned[64:]


def gather_sum(x):
    return pl.pallas_call(
        gather_sum_kernel,
        out_shape=jax.ShapeDtypeStruct((64, ROWS), jnp.bfloat16),
        compiler_params=room(12),
        in_specs=[VMEM],
        out_specs=VMEM,
        name="gather_sum",
    )(*on_chip(x))


def shards(
    queries,
    key_states,
    value_states,
    doc_lengths,
    move_plan,
    expert_ids,
    gate_weights,
    expert_weight,
):
    dp_size = lax.axis_size("dp")
    swap = [(0, 1), (1, 0)]
    weight = expert_weight.reshape(CHIPS, 2, WIDTH, FF)
    rows, row_load, w_own = attention(
        doc_lengths.T, move_plan.T, queries, key_states, value_states, weight, dp_size
    )
    own_rows = lax.all_to_all(
        jnp.broadcast_to(rows[None], (CHIPS, ROWS, WIDTH)), ("x", "y"), 0, 0
    )
    other_rows = lax.ppermute(own_rows, "c", swap)
    acc, gate, w_other, attended = own_half(
        own_rows, w_own, rows, weight, expert_ids.T, gate_weights.T
    )
    mine, theirs = other_half(other_rows, w_other, acc, gate)
    paired = pair_sum(mine, lax.ppermute(theirs, "c", swap))
    combined = gather_sum(lax.all_to_all(paired, ("x", "y"), 0, 0)).T
    return (attended, combined, row_load)


def solution(mesh):
    split = Mesh(mesh.devices.reshape(mesh.shape["dp"], 4, 2, 2), ("dp",) + GROUP)
    return jax.shard_map(
        shards,
        mesh=split,
        in_specs=(
            P("dp", GROUP),
            P("dp", GROUP),
            P("dp", GROUP),
            P(),
            P(),
            P("dp", None),
            P("dp", None),
            P(GROUP, None, None),
        ),
        out_specs=(P("dp", GROUP), P("dp", GROUP), P("dp")),
        check_vma=False,
    )
```
